32 devices in a mesh: grp: 4 (over z), gx: 8 (over y, x, core).
Axes of the slice: x: 2, y: 2, z: 4, core: 2. Of those that a mesh axis runs over, the one named last changes fastest.
Arguments:
- component_density: float32 [53, 256, 1024], P(None, 'gx', 'grp'), may hold values from 0.05 to 2
- scaled_thermal_state: float32 [256, 1024], P('gx', 'grp'), may hold values from 0.5 to 1.5
- leading_direction_flow: float32 [256, 1024], P('gx', 'grp'), may hold values from -1 to 1
- trailing_direction_flow: float32 [256, 1024], P('gx', 'grp'), may hold values from -1 to 1
- spreading_coefficient: float32 [54], replicated, may hold values from 0.02 to 0.2
- colliding_pair: int32 [325, 2], replicated, may hold values from 0 to 52
- natural_exponent_scaler: float32 [325], replicated, may hold values from -3 to -1
- arrhenius_energy: float32 [325], replicated, may hold values from 0 to 2
- stoichiometric_output: float32 [325, 53], replicated, may hold values from 0.004 to 0.075
- formation_warming: float32 [53], replicated, may hold values from -1.8 to 1.8
- explicit_increments: int32 [2048], P(('grp', 'gx')), may hold values from 1 to 4, as said below
Outputs:
- species_out: float32 [53, 256, 1024], P(None, 'gx', 'grp')
- temperature_out: float32 [256, 1024], P('gx', 'grp')
The draws below stay inside these ranges and needn't reach their ends.
Inputs may be any that keep to these rules, and one draw needn't show every extreme that they name: `explicit_increments`: substep counts of the tiles, in the order of the tiles described in the reference program.
All inputs are finite; a program needn't handle non-finite values.
Results may differ from the reference program's by a relative error of at most 0.0003.
Values sent between devices are 32-bit elements; how exact they have to be, the bound alone decides.
A program may use at most 64 MiB of HBM per device.

```python
import math
import jax
import jax.numpy as jnp
from jax import lax

SPEC = 53
RXN = 325
CX = 32
CY = 256
TILE = 128
MINSUB = 1
MAXSUB = 4
GRID_LENGTH_LEAD = 256
GRID_LENGTH_TRAIL = 1024
TD = 64
TILES = 2048
N_GRP = 4
N_GX = 8


def draw_explicit_increments(key, part):
    device_count = TILES // TD
    hot_key, drawn_key, busy_key, place_key = jax.random.split(key, 4)
    heated = jax.random.randint(hot_key, (device_count, 1), 0, 8) == 0
    drawn = jax.random.randint(drawn_key, (device_count, TD), MINSUB, MINSUB + 2)
    busy = jax.random.randint(busy_key, (device_count, TD), MAXSUB - 1, MAXSUB + 1)
    tallies = jnp.where(heated, busy, drawn).reshape(TILES)
    spots = jax.random.randint(place_key, (1,), 0, TILES)
    tallies = tallies.at[spots[0]].set(MAXSUB)
    other_spot = (spots[0] + TD) % TILES
    tallies = tallies.at[other_spot].set(MINSUB)
    return tallies.astype(jnp.int32)


def touch_ends(values, stream_key, smallest, high):
    longest = values.shape.index(max(values.shape))
    spots = []
    for shift in (0, 1):
        where = [jax.random.randint(jax.random.fold_in(stream_key, axis), (), 0, length) for axis, length in enumerate(values.shape)]
        where[longest] = (where[longest] + shift) % values.shape[longest]
        spots.append(tuple(where))
    return values.at[spots[0]].set(smallest).at[spots[1]].set(high)


def levels(own_key, dims, pieces, low, largest):
    loudness, own = 1.0, jax.random.fold_in(own_key, 6)
    for axis_at, blocks in pieces:
        heights = jnp.exp(jax.random.uniform(jax.random.fold_in(own, axis_at), (blocks,), jnp.float32, low / len(pieces), largest / len(pieces)))
        loudness = loudness * jnp.repeat(heights, dims[axis_at] // blocks).reshape([-1 if axis == axis_at else 1 for axis in range(len(dims))])
    return loudness


def normal_values(stream_key, shape, scale, limit, held_as=jnp.bfloat16):
    array = scale * jax.random.normal(stream_key, shape, jnp.float32)
    return jnp.clip(array, min=-limit, max=limit).astype(held_as)


def setup_inputs(seed: int = 0) -> dict:
    splits = jax.random.split(jax.random.key(seed), 12)
    return {
        "component_density": jnp.clip(jnp.exp(math.log(2.0) - 3.6888794 * jax.random.uniform(splits[0], (SPEC, GRID_LENGTH_LEAD, GRID_LENGTH_TRAIL), jnp.float32) ** levels(splits[0], (SPEC, GRID_LENGTH_LEAD, GRID_LENGTH_TRAIL), ((1, 8), (2, 4)), -0.2, 0.2)), 0.05, 2.0),
        "scaled_thermal_state": jnp.clip(0.5 + 1.0 * jax.random.uniform(splits[1], (GRID_LENGTH_LEAD, GRID_LENGTH_TRAIL), jnp.float32) ** levels(splits[1], (GRID_LENGTH_LEAD, GRID_LENGTH_TRAIL), ((0, 8), (1, 4)), -0.2, 0.2), 0.5, 1.5),
        "leading_direction_flow": jnp.clip(jax.random.uniform(splits[2], (GRID_LENGTH_LEAD, GRID_LENGTH_TRAIL), jnp.float32, -1.0, 1.0) * levels(splits[2], (GRID_LENGTH_LEAD, GRID_LENGTH_TRAIL), ((0, 8), (1, 4)), -0.4, 0.0), -1.0, 1.0),
        "trailing_direction_flow": jnp.clip(jax.random.uniform(splits[3], (GRID_LENGTH_LEAD, GRID_LENGTH_TRAIL), jnp.float32, -1.0, 1.0) * levels(splits[3], (GRID_LENGTH_LEAD, GRID_LENGTH_TRAIL), ((0, 8), (1, 4)), -0.4, 0.0), -1.0, 1.0),
        "spreading_coefficient": jnp.clip(jnp.exp(jax.random.uniform(splits[4], (SPEC + 1,), jnp.float32, math.log(0.02), math.log(0.2))), 0.02, 0.2),
        "colliding_pair": touch_ends(jax.random.randint(splits[5], (RXN, 2), 0, SPEC), jax.random.fold_in(splits[5], 1), 0, SPEC - 1).astype(jnp.int32),
        "natural_exponent_scaler": jnp.clip(jax.random.uniform(splits[6], (RXN,), jnp.float32, -3.0, -1.0), -3.0, -1.0),
        "arrhenius_energy": jnp.clip(jax.random.uniform(splits[7], (RXN,), jnp.float32, 0.0, 2.0), 0.0, 2.0),
        "stoichiometric_output": jnp.clip(jnp.exp(jax.random.uniform(splits[8], (RXN, SPEC), jnp.float32, math.log(0.004), math.log(0.075))), 0.004, 0.075),
        "formation_warming": normal_values(splits[9], (SPEC,), 0.3, 1.8, jnp.float32),
        "explicit_increments": draw_explicit_increments(jax.random.fold_in(splits[11], 71), 0),
    }


transport_step = 0.4
chemistry_span = 0.5
sixth_first = (0.75, -0.15, 1.0 / 60.0)
sixth_second = (1.5, -0.15, 1.0 / 90.0)
sixth_center = -49.0 / 18.0


def tendency(extended, speeds, spreading_coefficient):
    height = extended.shape[1] - 6
    breadth = extended.shape[2] - 6

    def along_first(values, offset):
        return values[:, 3 + offset:3 + offset + height, 3:3 + breadth]

    def along_second(values, offset):
        return values[:, 3:3 + height, 3 + offset:3 + offset + breadth]

    east_flux = speeds[0:1] * extended
    north_flux = speeds[1:2] * extended
    gradient = jnp.zeros((extended.shape[0], height, breadth), jnp.float32)
    laplacian = 2.0 * sixth_center * along_first(extended, 0)
    for offset in range(1, 4):
        gradient = gradient + sixth_first[offset - 1] * (along_first(east_flux, offset) - along_first(east_flux, -offset) + along_second(north_flux, offset) - along_second(north_flux, -offset))
        laplacian = laplacian + sixth_second[offset - 1] * (along_first(extended, offset) + along_first(extended, -offset) + along_second(extended, offset) + along_second(extended, -offset))
    return spreading_coefficient[:, None, None] * laplacian - gradient


def build_tables(colliding_pair, stoichiometric_output):
    species_ids = jnp.arange(stoichiometric_output.shape[1], dtype=jnp.int32)[:, None]
    first_table = (species_ids == colliding_pair[None, :, 0]).astype(jnp.float32)
    second_table = (species_ids == colliding_pair[None, :, 1]).astype(jnp.float32)
    return stoichiometric_output.T, jnp.concatenate([first_table, second_table], 1)


def substep_once(combined_state_array, step_sizes, mechanism):
    gain_table, loss_table, colliding_pair, natural_exponent_scaler, arrhenius_energy, formation_warming = mechanism
    amounts = combined_state_array[:-1]
    warmth = combined_state_array[-1]
    rate_constant = jnp.exp(natural_exponent_scaler[:, None] + arrhenius_energy[:, None] * jnp.tanh(warmth)[None, :])
    first_partner = jnp.take(amounts, colliding_pair[:, 0], axis=0)
    second_partner = jnp.take(amounts, colliding_pair[:, 1], axis=0)
    progress = rate_constant * first_partner * second_partner
    gained = jnp.dot(gain_table, progress, precision=lax.Precision.HIGHEST, preferred_element_type=jnp.float32)
    partners = jnp.concatenate([rate_constant * second_partner, rate_constant * first_partner], 0)
    destroyed = jnp.dot(loss_table, partners, precision=lax.Precision.HIGHEST, preferred_element_type=jnp.float32)
    updated = (amounts + step_sizes[None, :] * gained) / (1.0 + step_sizes[None, :] * destroyed)
    warmer = warmth + jnp.dot(formation_warming, updated - amounts, precision=lax.Precision.HIGHEST, preferred_element_type=jnp.float32)
    return jnp.concatenate([updated, warmer[None, :]], 0)


def substep_loop(combined_state_array, counts, turn_count, mechanism):
    step_sizes = chemistry_span / counts.astype(jnp.float32)

    def advance(substep, current):
        advanced = substep_once(current, step_sizes, mechanism)
        return jnp.where((substep < counts)[None, :], advanced, current)

    return lax.fori_loop(0, turn_count, advance, combined_state_array)


def periodic(values):
    return jnp.pad(values, ((0, 0), (3, 3), (3, 3)), mode="wrap")


def reference(component_density, scaled_thermal_state, leading_direction_flow, trailing_direction_flow, spreading_coefficient, colliding_pair, natural_exponent_scaler, arrhenius_energy, stoichiometric_output, formation_warming, explicit_increments):
    combined_state_array = jnp.concatenate([component_density, scaled_thermal_state[None]], 0)
    speed_wide = periodic(jnp.stack([leading_direction_flow, trailing_direction_flow]))
    section_one = combined_state_array + transport_step * tendency(periodic(combined_state_array), speed_wide, spreading_coefficient)
    section_two = 0.75 * combined_state_array + 0.25 * (section_one + transport_step * tendency(periodic(section_one), speed_wide, spreading_coefficient))
    advected = combined_state_array / 3.0 + (2.0 / 3.0) * (section_two + transport_step * tendency(periodic(section_two), speed_wide, spreading_coefficient))
    clipped = jnp.concatenate([jnp.maximum(advected[:-1], 0.0), advected[-1:]], 0)
    layers = SPEC + 1
    blocks = clipped.reshape(layers, N_GX, CX, N_GRP, CY).transpose(3, 1, 0, 2, 4).reshape(N_GRP * N_GX, layers, CX * CY)
    cell_counts = jnp.repeat(explicit_increments.reshape(N_GRP * N_GX, -1), TILE, axis=1)
    gain_table, loss_table = build_tables(colliding_pair, stoichiometric_output)
    mechanism = (gain_table, loss_table, colliding_pair, natural_exponent_scaler, arrhenius_energy, formation_warming)

    def per_device(device_pair):
        device_block, device_counts = device_pair
        return substep_loop(device_block, device_counts, MAXSUB, mechanism)

    reacted = lax.map(per_device, (blocks, cell_counts))
    restored = reacted.reshape(N_GRP, N_GX, layers, CX, CY).transpose(2, 1, 3, 0, 4).reshape(layers, GRID_LENGTH_LEAD, GRID_LENGTH_TRAIL)
    return restored[:SPEC], restored[SPEC]
```

```python
import functools
import math

import jax
import jax.numpy as jnp
from jax import lax
from jax.experimental import pallas as pl
from jax.experimental.pallas import tpu as pltpu
from jax.sharding import PartitionSpec as P

TILE = 128
HALO = 9
FIRST_SCALE = 60.0
SECOND_SCALE = 180.0
transport_step = 0.4
chemistry_span = 0.5
sixth_first = (0.75, -0.15, 1.0 / 60.0)
sixth_second = (1.5, -0.15, 1.0 / 90.0)
sixth_center = -49.0 / 18.0


def up8(n):
    return -(-n // 8) * 8


def halves(value):
    high = value.astype(jnp.bfloat16)
    return high, (value - high.astype(jnp.float32)).astype(jnp.bfloat16)


def transport_kernel(fields, main, top, bottom, side, diff, band, uv_main, uv_top, uv_bottom, uv_side,
                     out, start, one, two, east, north, pieces, across):
    rows, _, cols = main.shape
    wide = rows + 2 * HALO
    gap = side.shape[2]
    width = cols + gap
    tile = pl.program_id(0)
    u_at, v_at = fields % 8, (fields + 1) % 8

    def fill(dst, m, t, b, s, sub):
        def put(r, ref, at):
            if sub is None:
                dst[r, :, :cols] = ref[at]
            else:
                dst[r, :, :cols] = jnp.broadcast_to(ref[at, sub:sub + 1, :], (8, cols))

        def mid(r, c):
            put(HALO + r, m, r)
            return c

        lax.fori_loop(0, rows, mid, 0, unroll=4)
        for r in range(HALO):
            put(r, t, r)
            put(HALO + rows + r, b, r)

        def edge(r, c):
            if sub is None:
                dst[r, :, cols:] = s[r]
            else:
                dst[r, :, cols:] = jnp.broadcast_to(s[r, sub:sub + 1, :], (8, gap))
            return c

        lax.fori_loop(0, wide, edge, 0, unroll=5)

    @pl.when(tile == 0)
    def _():
        fill(east, uv_main, uv_top, uv_bottom, uv_side, u_at)
        fill(north, uv_main, uv_top, uv_bottom, uv_side, v_at)

    fill(start, main, top, bottom, side, None)
    d = diff[...] * transport_step
    d_wide = jnp.concatenate([d] * (width // 128), axis=1)

    def columns(src, low, high):
        scale = d_wide * (1.0 / SECOND_SCALE)

        def split(j, c):
            fs, gs = [], []
            for q in range(2):
                i = low + 2 * j + q
                f = src[i]
                fs.append(scale * f)
                gs.append((-transport_step / FIRST_SCALE) * (north[i] * f))
            f_high, f_low = halves(jnp.concatenate(fs, 0))
            g_high, g_low = halves(jnp.concatenate(gs, 0))
            at = pl.ds(pl.multiple_of(j * 16, 16), 16)
            pieces[at, 0:width] = f_high
            pieces[at, width:2 * width] = f_low
            pieces[at, 2 * width:3 * width] = g_high
            pieces[at, 3 * width:4 * width] = g_low
            return c

        lax.fori_loop(0, (high - low) // 2, split, 0, unroll=2 if (high - low) % 4 == 0 else 1)
        count = (high - low) * 8
        across[0:count] = jnp.dot(pieces[0:count], band[...], preferred_element_type=jnp.float32)

    def change(src, i, low, n):
        lap = sixth_center * src[i, :, :n]
        grad = None
        for k in range(1, 4):
            ahead, behind = src[i + k, :, :n], src[i - k, :, :n]
            lap = lap + sixth_second[k - 1] * (ahead + behind)
            slope = (sixth_first[k - 1] * transport_step) * (
                east[i + k, :, :n] * ahead - east[i - k, :, :n] * behind)
            grad = slope if grad is None else grad + slope
        col = across[pl.ds(pl.multiple_of((i - low) * 8, 8), 8), :n]
        return col + (d_wide[:, :n] * lap - grad)

    columns(start, 3, wide - 3)

    def first(i, c):
        one[i] = start[i] + change(start, i, 3, width)
        return c

    lax.fori_loop(3, wide - 3, first, 0, unroll=2)
    columns(one, 6, wide - 6)

    def second(i, c):
        two[i] = 0.75 * start[i] + 0.25 * (one[i] + change(one, i, 6, width))
        return c

    lax.fori_loop(6, wide - 6, second, 0, unroll=2)
    columns(two, 9, wide - 9)
    ids = tile * 8 + lax.broadcasted_iota(jnp.int32, (8, cols), 0)
    is_species = ids < fields - 1

    def third(i, c):
        value = start[i, :, :cols] * (1.0 / 3.0) + (2.0 / 3.0) * (
            two[i, :, :cols] + change(two, i, 9, cols))
        out[i - HALO] = jnp.where(is_species, jnp.maximum(value, 0.0), value)
        return c

    lax.fori_loop(9, wide - 9, third, 0, unroll=2)


def band_matrix(width):
    here = jnp.arange(width, dtype=jnp.int32)
    lag = (here[:, None] - here[None, :]) % width
    second = jnp.zeros((width, width), jnp.float32)
    first = jnp.zeros((width, width), jnp.float32)
    second = jnp.where(lag == 0, round(sixth_center * SECOND_SCALE), second)
    for k in range(1, 4):
        ahead, behind = lag == k, lag == width - k
        second = jnp.where(ahead | behind, round(sixth_second[k - 1] * SECOND_SCALE), second)
        weight = round(sixth_first[k - 1] * FIRST_SCALE)
        first = jnp.where(ahead, weight, jnp.where(behind, -weight, first))
    return jnp.concatenate([second, second, first, first], 0).astype(jnp.bfloat16)


def transport(main, top, bottom, side, diff, fields):
    rows, layers, cols = main.shape
    wide = rows + 2 * HALO
    gap = side.shape[2]
    width = cols + gap
    uv_tile = fields // 8
    band = band_matrix(width)
    by = lambda r, n: pl.BlockSpec((r, 8, n), lambda t: (0, t, 0))
    uv = lambda r, n: pl.BlockSpec((r, 8, n), lambda t: (0, uv_tile, 0))
    return pl.pallas_call(
        functools.partial(transport_kernel, fields),
        grid=(layers // 8,),
        in_specs=[by(rows, cols), by(HALO, cols), by(HALO, cols), by(wide, gap),
                  pl.BlockSpec((8, 128), lambda t: (t, 0)),
                  pl.BlockSpec(band.shape, lambda t: (0, 0)),
                  uv(rows, cols), uv(HALO, cols), uv(HALO, cols), uv(wide, gap)],
        out_specs=by(rows, cols),
        out_shape=jax.ShapeDtypeStruct(main.shape, jnp.float32),
        scratch_shapes=[pltpu.VMEM((wide, 8, width), jnp.float32) for _ in range(5)]
        + [pltpu.VMEM(((wide - 6) * 8, 4 * width), jnp.bfloat16),
           pltpu.VMEM(((wide - 6) * 8, width), jnp.float32)],
        name="transport",
    )(main, top, bottom, side, diff, band, main, top, bottom, side)


CHAINS = 2


def chemistry_kernel(reactions, warm_row, order, counts, state, gather, sums, prefactor, energy,
                     warming, out, *scratch):
    R = reactions
    rows, layers, cols = state.shape
    per_row = cols // TILE
    tiles = rows * per_row
    cells = 2 * TILE
    group = 2 * CHAINS
    is_warm = lax.broadcasted_iota(jnp.int32, (layers, 1), 0) == warm_row
    second_half = lax.broadcasted_iota(jnp.int32, (1, cells), 1) >= TILE
    values, partners, parts = scratch[:CHAINS], scratch[CHAINS:2 * CHAINS], scratch[2 * CHAINS:]

    def handle(g, c):
        ids = [order[g * group + t] for t in range(group)]
        places = [(t // per_row, pl.ds(pl.multiple_of((t % per_row) * TILE, TILE), TILE)) for t in ids]
        numbers = [counts[t] for t in ids]
        turn_count = functools.reduce(jnp.maximum, numbers)
        steps, cell_counts = [], []
        for q in range(CHAINS):
            n = jnp.where(second_half, numbers[2 * q + 1], numbers[2 * q])
            cell_counts.append(n)
            steps.append(chemistry_span / n.astype(jnp.float32))
            for t in range(2):
                r, at = places[2 * q + t]
                values[q][:, t * TILE:(t + 1) * TILE] = state[r, :, at]

        def advance(s, c):
            for q in range(CHAINS):
                high, low = halves(values[q][...])
                pieces = jnp.concatenate(
                    [high.astype(jnp.float32), low.astype(jnp.float32)], 0).astype(jnp.bfloat16)
                partners[q][...] = jnp.dot(gather[...], pieces, preferred_element_type=jnp.float32)
            for q in range(CHAINS):
                heat = jnp.tanh(values[q][warm_row:warm_row + 1, :])
                for r in range(0, R, 16):
                    block = pl.ds(r, 16)
                    a = jnp.concatenate([prefactor[block]] * 2, 1)
                    e = jnp.concatenate([energy[block]] * 2, 1)
                    rate = jnp.exp2(a + e * heat)
                    ca = partners[q][block]
                    cb = partners[q][pl.ds(R + r, 16)]
                    qa = rate * ca
                    qb = rate * cb
                    p = qa * cb
                    for n, value in enumerate((p, qb, qa)):
                        hi, lo = halves(value)
                        parts[q][pl.ds(2 * n * R + r, 16)] = hi
                        parts[q][pl.ds((2 * n + 1) * R + r, 16)] = lo
            for q in range(CHAINS):
                x = values[q][...]
                h = steps[q]
                both = jnp.dot(sums[0:2 * layers, 0:2 * R], parts[q][0:2 * R],
                               preferred_element_type=jnp.float32)
                destroyed = jnp.dot(sums[0:layers, 2 * R:], parts[q][2 * R:],
                                    preferred_element_type=jnp.float32)
                gained = both[:layers] + both[layers:]
                updated = (x + h * gained) / (1.0 + h * destroyed)
                change = jnp.sum(warming[...][:, 0:1] * (updated - x), axis=0, keepdims=True)
                updated = jnp.where(is_warm, x + change, updated)
                values[q][...] = jnp.where(s < cell_counts[q], updated, x)
            return c

        lax.fori_loop(0, turn_count, advance, 0)
        for q in range(CHAINS):
            for t in range(2):
                r, at = places[2 * q + t]
                out[r, :, at] = values[q][:, t * TILE:(t + 1) * TILE]
        return c

    lax.fori_loop(0, tiles // group, handle, 0)


def chemistry(state, order, counts, tables):
    rows, layers, cols = state.shape
    gather, sums, prefactor, energy, warming, warm_row = tables
    R = prefactor.shape[0]
    smem = pl.BlockSpec(memory_space=pltpu.SMEM)
    vmem = pl.BlockSpec(memory_space=pltpu.VMEM)
    return pl.pallas_call(
        functools.partial(chemistry_kernel, R, warm_row),
        in_specs=[smem, smem] + [vmem] * 6,
        out_specs=vmem,
        out_shape=jax.ShapeDtypeStruct(state.shape, jnp.float32),
        scratch_shapes=[pltpu.VMEM((layers, 2 * TILE), jnp.float32)] * CHAINS
        + [pltpu.VMEM((2 * R, 2 * TILE), jnp.float32)] * CHAINS
        + [pltpu.VMEM((6 * R, 2 * TILE), jnp.bfloat16)] * CHAINS,
        name="chemistry",
    )(order, counts, state, gather, sums, prefactor, energy, warming)


def by_count(counts):
    tiles = counts.shape[0]
    ids = jnp.arange(tiles, dtype=jnp.int32)
    key = counts * tiles + ids
    rank = jnp.sum((key[None, :] < key[:, None]).astype(jnp.int32), 1)
    return jnp.sum(jnp.where(rank[:, None] == ids[None, :], ids[:, None], 0), 0)


def build_tables(colliding_pair, prefactor, energy, produced, warming, layers):
    reactions, species = produced.shape
    R = -(-reactions // 16) * 16
    pad = R - reactions
    ids = jnp.arange(layers, dtype=jnp.int32)
    pair = jnp.pad(colliding_pair, ((0, pad), (0, 0)), constant_values=-1)
    first = (pair[:, 0:1] == ids[None]).astype(jnp.bfloat16)
    second = (pair[:, 1:2] == ids[None]).astype(jnp.bfloat16)
    both = jnp.concatenate([first, second], 0)
    gather = jnp.concatenate([both, both], 1)
    gain = jnp.pad(produced.T, ((0, layers - species), (0, pad)))
    gain_high = lax.reduce_precision(gain, 8, 7)
    gain_low = (gain - gain_high).astype(jnp.bfloat16)
    gain_high = gain_high.astype(jnp.bfloat16)
    zero = jnp.zeros_like(gain_high)
    one = jnp.concatenate([gain_high, gain_high, first.T, first.T, second.T, second.T], 1)
    low = jnp.concatenate([gain_low, zero, zero, zero, zero, zero], 1)
    sums = jnp.concatenate([one, low], 0)
    scale = 1.0 / math.log(2.0)
    wide = lambda v: jnp.broadcast_to(jnp.pad(v * scale, (0, pad))[:, None], (R, 128))
    heats = jnp.broadcast_to(jnp.pad(warming, (0, layers - species))[:, None], (layers, 128))
    return gather, sums, wide(prefactor), wide(energy), heats, species


def body(component_density, scaled_thermal_state, leading_direction_flow, trailing_direction_flow,
         spreading_coefficient, colliding_pair, natural_exponent_scaler, arrhenius_energy,
         stoichiometric_output, formation_warming, explicit_increments):
    species, rows, cols = component_density.shape
    fields = species + 1
    layers = up8(fields + 2)
    bundle = jnp.concatenate(
        [component_density, scaled_thermal_state[None], leading_direction_flow[None],
         trailing_direction_flow[None]], 0)
    bundle = jnp.pad(bundle, ((0, layers - fields - 2), (0, 0), (0, 0)))
    main = jnp.transpose(bundle, (1, 0, 2))

    def ring(axis):
        n = lax.axis_size(axis)
        return [(i, (i + 1) % n) for i in range(n)], [((i + 1) % n, i) for i in range(n)]

    up, down = ring("gx")
    top = lax.ppermute(main[rows - HALO:], "gx", up)
    bottom = lax.ppermute(main[:HALO], "gx", down)
    tall = jnp.concatenate(
        [top[:, :, :HALO], main[:, :, :HALO], bottom[:, :, :HALO]], 0)
    tall_end = jnp.concatenate(
        [top[:, :, cols - HALO:], main[:, :, cols - HALO:], bottom[:, :, cols - HALO:]], 0)
    up, down = ring("grp")
    left = lax.ppermute(jnp.transpose(tall_end, (2, 0, 1)), "grp", up)
    right = lax.ppermute(jnp.transpose(tall, (2, 0, 1)), "grp", down)
    gap = jnp.zeros((128 - 2 * HALO,) + left.shape[1:], jnp.float32)
    side = jnp.transpose(jnp.concatenate([right, gap, left], 0), (1, 2, 0))
    diff = jnp.broadcast_to(
        jnp.pad(spreading_coefficient, (0, layers - fields))[:, None], (layers, 128))
    clipped = transport(main, top, bottom, side, diff, fields)
    tables = build_tables(colliding_pair, natural_exponent_scaler, arrhenius_energy,
                          stoichiometric_output, formation_warming, layers)
    reacted = chemistry(clipped, by_count(explicit_increments), explicit_increments, tables)
    species_out = jnp.transpose(reacted[:, :species], (1, 0, 2))
    return species_out, reacted[:, species]


def solution(mesh):
    return jax.shard_map(
        body,
        mesh=mesh,
        in_specs=(
            P(None, "gx", "grp"),
            P("gx", "grp"),
            P("gx", "grp"),
            P("gx", "grp"),
            P(),
            P(),
            P(),
            P(),
            P(),
            P(),
            P(("grp", "gx")),
        ),
        out_specs=(P(None, "gx", "grp"), P("gx", "grp")),
        check_vma=False,
    )
```

```python
import functools
import math

import jax
import jax.numpy as jnp
import numpy as np
from jax import lax
from jax.experimental import pallas as pl
from jax.experimental.pallas import tpu as pltpu
from jax.sharding import PartitionSpec as P

TILE = 128
HALO = 9
FIRST_SCALE = 60.0
SECOND_SCALE = 180.0
transport_step = 0.4
chemistry_span = 0.5
sixth_first = (0.75, -0.15, 1.0 / 60.0)
sixth_second = (1.5, -0.15, 1.0 / 90.0)
sixth_center = -49.0 / 18.0


def up8(n):
    return -(-n // 8) * 8


def halo_kernel(sizes, main, first_cols, last_cols, top, bottom, left, right, send, recv):
    n_grp, n_gx = sizes
    g, x = lax.axis_index("grp"), lax.axis_index("gx")
    rows = main.shape[0]
    place = lambda dg, dx: (lax.rem(g + dg + n_grp, n_grp), lax.rem(x + dx + n_gx, n_gx))
    barrier = pltpu.get_barrier_semaphore()
    around = [(dg, dx) for dg in (-1, 0, 1) for dx in (-1, 0, 1) if (dg, dx) != (0, 0)]
    for dg, dx in around:
        pl.semaphore_signal(barrier, inc=1, device_id=place(dg, dx),
                            device_id_type=pl.DeviceIdType.MESH)
    pl.semaphore_wait(barrier, len(around))
    early, late = pl.ds(0, HALO), pl.ds(rows - HALO, HALO)
    above, beside, below = pl.ds(0, HALO), pl.ds(HALO, rows), pl.ds(HALO + rows, HALO)
    plan = [
        (main.at[late], top, 0, 1),
        (main.at[early], bottom, 0, -1),
        (last_cols, left.at[beside], 1, 0),
        (first_cols, right.at[beside], -1, 0),
        (last_cols.at[late], left.at[above], 1, 1),
        (last_cols.at[early], left.at[below], 1, -1),
        (first_cols.at[late], right.at[above], -1, 1),
        (first_cols.at[early], right.at[below], -1, -1),
    ]
    copies = []
    for n, (src, dst, dg, dx) in enumerate(plan):
        copy = pltpu.make_async_remote_copy(
            src_ref=src, dst_ref=dst, send_sem=send.at[n], recv_sem=recv.at[n],
            device_id=place(dg, dx), device_id_type=pl.DeviceIdType.MESH)
        copy.start()
        copies.append(copy)
    for copy in copies:
        copy.wait()


def exchange(main, first_cols, last_cols):
    rows, layers, cols = main.shape
    sizes = (lax.axis_size("grp"), lax.axis_size("gx"))
    anywhere = pl.BlockSpec(memory_space=pltpu.VMEM)
    strip = jax.ShapeDtypeStruct((HALO, layers, cols), jnp.float32)
    edge = jax.ShapeDtypeStruct((rows + 2 * HALO,) + first_cols.shape[1:], jnp.float32)
    return pl.pallas_call(
        functools.partial(halo_kernel, sizes),
        in_specs=[anywhere] * 3,
        out_specs=[anywhere] * 4,
        out_shape=[strip, strip, edge, edge],
        scratch_shapes=[pltpu.SemaphoreType.DMA((8,)), pltpu.SemaphoreType.DMA((8,))],
        compiler_params=pltpu.CompilerParams(collective_id=0, has_side_effects=True),
        name="halo",
    )(main, first_cols, last_cols)


def halves(value):
    high = value.astype(jnp.bfloat16)
    return high, (value - high.astype(jnp.float32)).astype(jnp.bfloat16)


def transport_kernel(fields, main, top, bottom, side, diff, band, uv_main, uv_top, uv_bottom, uv_side,
                     out, start, one, two, east, north, pieces, across):
    rows, _, cols = main.shape
    wide = rows + 2 * HALO
    gap = side.shape[2]
    width = cols + gap
    tile = pl.program_id(0)
    u_at, v_at = fields % 8, (fields + 1) % 8

    def fill(dst, m, t, b, s, sub):
        def put(r, ref, at):
            if sub is None:
                dst[r, :, :cols] = ref[at]
            else:
                dst[r, :, :cols] = jnp.broadcast_to(ref[at, sub:sub + 1, :], (8, cols))

        def mid(r, c):
            put(HALO + r, m, r)
            return c

        lax.fori_loop(0, rows, mid, 0, unroll=4)
        for r in range(HALO):
            put(r, t, r)
            put(HALO + rows + r, b, r)

        def edge(r, c):
            if sub is None:
                dst[r, :, cols:] = s[r]
            else:
                dst[r, :, cols:] = jnp.broadcast_to(s[r, sub:sub + 1, :], (8, gap))
            return c

        lax.fori_loop(0, wide, edge, 0, unroll=5)

    @pl.when(tile == 0)
    def _():
        fill(east, uv_main, uv_top, uv_bottom, uv_side, u_at)
        fill(north, uv_main, uv_top, uv_bottom, uv_side, v_at)

    fill(start, main, top, bottom, side, None)
    d = diff[...] * transport_step
    d_wide = jnp.concatenate([d] * (width // 128), axis=1)

    def columns(src, low, high):
        scale = d_wide * (1.0 / SECOND_SCALE)

        def split(j, c):
            fs, gs = [], []
            for q in range(2):
                i = low + 2 * j + q
                f = src[i]
                fs.append(scale * f)
                gs.append((-transport_step / FIRST_SCALE) * (north[i] * f))
            f_high, f_low = halves(jnp.concatenate(fs, 0))
            g_high, g_low = halves(jnp.concatenate(gs, 0))
            at = pl.ds(pl.multiple_of(j * 16, 16), 16)
            pieces[at, 0:width] = f_high
            pieces[at, width:2 * width] = f_low
            pieces[at, 2 * width:3 * width] = g_high
            pieces[at, 3 * width:4 * width] = g_low
            return c

        lax.fori_loop(0, (high - low) // 2, split, 0, unroll=2 if (high - low) % 4 == 0 else 1)
        count = (high - low) * 8
        across[0:count] = jnp.dot(pieces[0:count], band[...], preferred_element_type=jnp.float32)

    def change(src, i, low, n):
        lap = sixth_center * src[i, :, :n]
        grad = None
        for k in range(1, 4):
            ahead, behind = src[i + k, :, :n], src[i - k, :, :n]
            lap = lap + sixth_second[k - 1] * (ahead + behind)
            slope = (sixth_first[k - 1] * transport_step) * (
                east[i + k, :, :n] * ahead - east[i - k, :, :n] * behind)
            grad = slope if grad is None else grad + slope
        col = across[pl.ds(pl.multiple_of((i - low) * 8, 8), 8), :n]
        return col + (d_wide[:, :n] * lap - grad)

    columns(start, 3, wide - 3)

    def first(i, c):
        one[i] = start[i] + change(start, i, 3, width)
        return c

    lax.fori_loop(3, wide - 3, first, 0, unroll=2)
    columns(one, 6, wide - 6)

    def second(i, c):
        two[i] = 0.75 * start[i] + 0.25 * (one[i] + change(one, i, 6, width))
        return c

    lax.fori_loop(6, wide - 6, second, 0, unroll=2)
    columns(two, 9, wide - 9)
    ids = tile * 8 + lax.broadcasted_iota(jnp.int32, (8, cols), 0)
    is_species = ids < fields - 1

    def third(i, c):
        value = start[i, :, :cols] * (1.0 / 3.0) + (2.0 / 3.0) * (
            two[i, :, :cols] + change(two, i, 9, cols))
        out[i - HALO] = jnp.where(is_species, jnp.maximum(value, 0.0), value)
        return c

    lax.fori_loop(9, wide - 9, third, 0, unroll=2)


def band_matrix(width):
    here = np.arange(width)
    lag = (here[:, None] - here[None, :]) % width
    second = np.where(lag == 0, round(sixth_center * SECOND_SCALE), 0)
    first = np.zeros((width, width))
    for k in range(1, 4):
        ahead, behind = lag == k, lag == width - k
        second = np.where(ahead | behind, round(sixth_second[k - 1] * SECOND_SCALE), second)
        weight = round(sixth_first[k - 1] * FIRST_SCALE)
        first = np.where(ahead, weight, np.where(behind, -weight, first))
    return jnp.asarray(np.concatenate([second, second, first, first], 0), jnp.bfloat16)


def transport(main, top, bottom, side, diff, fields):
    rows, layers, cols = main.shape
    wide = rows + 2 * HALO
    gap = side.shape[2]
    width = cols + gap
    uv_tile = fields // 8
    band = band_matrix(width)
    by = lambda r, n: pl.BlockSpec((r, 8, n), lambda t: (0, t, 0))
    uv = lambda r, n: pl.BlockSpec((r, 8, n), lambda t: (0, uv_tile, 0))
    return pl.pallas_call(
        functools.partial(transport_kernel, fields),
        grid=(layers // 8,),
        in_specs=[by(rows, cols), by(HALO, cols), by(HALO, cols), by(wide, gap),
                  pl.BlockSpec((8, 128), lambda t: (t, 0)),
                  pl.BlockSpec(band.shape, lambda t: (0, 0)),
                  uv(rows, cols), uv(HALO, cols), uv(HALO, cols), uv(wide, gap)],
        out_specs=by(rows, cols),
        out_shape=jax.ShapeDtypeStruct(main.shape, jnp.float32),
        scratch_shapes=[pltpu.VMEM((wide, 8, width), jnp.float32) for _ in range(5)]
        + [pltpu.VMEM(((wide - 6) * 8, 4 * width), jnp.bfloat16),
           pltpu.VMEM(((wide - 6) * 8, width), jnp.float32)],
        name="transport",
    )(main, top, bottom, side, diff, band, main, top, bottom, side)


CHAINS = 2


def chemistry_kernel(reactions, warm_row, order, counts, state, gather, sums, prefactor, energy,
                     warming, out, warm_out, staged, sems, *scratch):
    R = reactions
    rows, layers, cols = state.shape
    per_row = cols // TILE
    tiles = rows * per_row
    cells = 2 * TILE
    group = 2 * CHAINS
    is_warm = lax.broadcasted_iota(jnp.int32, (layers, 1), 0) == warm_row
    second_half = lax.broadcasted_iota(jnp.int32, (1, cells), 1) >= TILE
    values, partners, parts = scratch[:CHAINS], scratch[CHAINS:2 * CHAINS], scratch[2 * CHAINS:]

    def handle(g, c):
        ids = [order[g * group + t] for t in range(group)]
        places = [(t // per_row, pl.ds(pl.multiple_of((t % per_row) * TILE, TILE), TILE)) for t in ids]
        numbers = [counts[t] for t in ids]
        turn_count = functools.reduce(jnp.maximum, numbers)
        steps, cell_counts = [], []
        for q in range(CHAINS):
            n = jnp.where(second_half, numbers[2 * q + 1], numbers[2 * q])
            cell_counts.append(n)
            steps.append(chemistry_span / n.astype(jnp.float32))
            for t in range(2):
                r, at = places[2 * q + t]
                values[q][:, t * TILE:(t + 1) * TILE] = state[r, :, at]

        def advance(s, c):
            for q in range(CHAINS):
                high, low = halves(values[q][...])
                pieces = jnp.concatenate(
                    [high.astype(jnp.float32), low.astype(jnp.float32)], 0).astype(jnp.bfloat16)
                partners[q][...] = jnp.dot(gather[...], pieces, preferred_element_type=jnp.float32)
            for q in range(CHAINS):
                heat = jnp.tanh(values[q][warm_row:warm_row + 1, :])
                for r in range(0, R, 16):
                    block = pl.ds(r, 16)
                    a = jnp.concatenate([prefactor[block]] * 2, 1)
                    e = jnp.concatenate([energy[block]] * 2, 1)
                    rate = jnp.exp2(a + e * heat)
                    ca = partners[q][block]
                    cb = partners[q][pl.ds(R + r, 16)]
                    qa = rate * ca
                    qb = rate * cb
                    p = qa * cb
                    for n, value in enumerate((p, qb, qa)):
                        hi, lo = halves(value)
                        parts[q][pl.ds(2 * n * R + r, 16)] = hi
                        parts[q][pl.ds((2 * n + 1) * R + r, 16)] = lo
            for q in range(CHAINS):
                x = values[q][...]
                h = steps[q]
                both = jnp.dot(sums[0:2 * layers, 0:2 * R], parts[q][0:2 * R],
                               preferred_element_type=jnp.float32)
                destroyed = jnp.dot(sums[0:layers, 2 * R:], parts[q][2 * R:],
                                    preferred_element_type=jnp.float32)
                gained = both[:layers] + both[layers:]
                updated = (x + h * gained) / (1.0 + h * destroyed)
                change = jnp.sum(warming[...][:, 0:1] * (updated - x), axis=0, keepdims=True)
                updated = jnp.where(is_warm, x + change, updated)
                values[q][...] = jnp.where(s < cell_counts[q], updated, x)
            return c

        lax.fori_loop(0, turn_count, advance, 0)
        for q in range(CHAINS):
            for t in range(2):
                r, at = places[2 * q + t]
                done = values[q][:, t * TILE:(t + 1) * TILE]
                for f in range(0, layers, 8):
                    n = min(8, warm_row + 1 - f)
                    if n > 0:
                        staged[pl.ds(((ids[2 * q + t] % per_row) * (warm_row + 1) + f) * rows + r, n, stride=rows)] = done[f:f + n]
        return c

    lax.fori_loop(0, tiles // group, handle, 0)
    height = (warm_row + 1) * rows
    copies = []
    for n in range(per_row):
        at = pl.ds(n * TILE, TILE)
        copies.append(pltpu.make_async_copy(
            staged.at[pl.ds(n * height, warm_row * rows)], out.at[:, at], sems.at[0, n]))
        copies.append(pltpu.make_async_copy(
            staged.at[pl.ds(n * height + warm_row * rows, rows)], warm_out.at[:, at], sems.at[1, n]))
    for copy in copies:
        copy.start()
    for copy in copies:
        copy.wait()


def chemistry(state, order, counts, tables):
    rows, layers, cols = state.shape
    gather, sums, prefactor, energy, warming, warm_row = tables
    R = prefactor.shape[0]
    smem = pl.BlockSpec(memory_space=pltpu.SMEM)
    vmem = pl.BlockSpec(memory_space=pltpu.VMEM)
    return pl.pallas_call(
        functools.partial(chemistry_kernel, R, warm_row),
        in_specs=[smem, smem] + [vmem] * 6,
        out_specs=[pl.BlockSpec(memory_space=pl.ANY)] * 2,
        out_shape=[jax.ShapeDtypeStruct((warm_row * rows, cols), jnp.float32),
                   jax.ShapeDtypeStruct((rows, cols), jnp.float32)],
        scratch_shapes=[pltpu.VMEM((cols // TILE * (warm_row + 1) * rows, TILE), jnp.float32),
                        pltpu.SemaphoreType.DMA((2, cols // TILE))]
        + [pltpu.VMEM((layers, 2 * TILE), jnp.float32)] * CHAINS
        + [pltpu.VMEM((2 * R, 2 * TILE), jnp.float32)] * CHAINS
        + [pltpu.VMEM((6 * R, 2 * TILE), jnp.bfloat16)] * CHAINS,
        name="chemistry",
    )(order, counts, state, gather, sums, prefactor, energy, warming)


def by_count(counts):
    tiles = counts.shape[0]
    ids = jnp.arange(tiles, dtype=jnp.int32)
    key = counts * tiles + ids
    rank = jnp.sum((key[None, :] < key[:, None]).astype(jnp.int32), 1)
    return jnp.sum(jnp.where(rank[:, None] == ids[None, :], ids[:, None], 0), 0)


def build_tables(colliding_pair, prefactor, energy, produced, warming, layers):
    reactions, species = produced.shape
    R = -(-reactions // 16) * 16
    pad = R - reactions
    ids = jnp.arange(layers, dtype=jnp.int32)
    pair = jnp.pad(colliding_pair, ((0, pad), (0, 0)), constant_values=-1)
    first = (pair[:, 0:1] == ids[None]).astype(jnp.bfloat16)
    second = (pair[:, 1:2] == ids[None]).astype(jnp.bfloat16)
    both = jnp.concatenate([first, second], 0)
    gather = jnp.concatenate([both, both], 1)
    gain = jnp.pad(produced.T, ((0, layers - species), (0, pad)))
    gain_high = lax.reduce_precision(gain, 8, 7)
    gain_low = (gain - gain_high).astype(jnp.bfloat16)
    gain_high = gain_high.astype(jnp.bfloat16)
    zero = jnp.zeros_like(gain_high)
    one = jnp.concatenate([gain_high, gain_high, first.T, first.T, second.T, second.T], 1)
    low = jnp.concatenate([gain_low, zero, zero, zero, zero, zero], 1)
    sums = jnp.concatenate([one, low], 0)
    scale = 1.0 / math.log(2.0)
    wide = lambda v: jnp.broadcast_to(jnp.pad(v * scale, (0, pad))[:, None], (R, 128))
    heats = jnp.broadcast_to(jnp.pad(warming, (0, layers - species))[:, None], (layers, 128))
    return gather, sums, wide(prefactor), wide(energy), heats, species


def body(component_density, scaled_thermal_state, leading_direction_flow, trailing_direction_flow,
         spreading_coefficient, colliding_pair, natural_exponent_scaler, arrhenius_energy,
         stoichiometric_output, formation_warming, explicit_increments):
    species, rows, cols = component_density.shape
    fields = species + 1
    layers = up8(fields + 2)
    bundle = jnp.concatenate(
        [component_density, scaled_thermal_state[None], leading_direction_flow[None],
         trailing_direction_flow[None]], 0)
    bundle = jnp.pad(bundle, ((0, layers - fields - 2), (0, 0), (0, 0)))
    main = jnp.transpose(bundle, (1, 0, 2))

    first_cols = jnp.transpose(main[:, :, :HALO], (0, 2, 1))
    last_cols = jnp.transpose(main[:, :, cols - HALO:], (0, 2, 1))
    top, bottom, left, right = exchange(main, first_cols, last_cols)
    gap = jnp.zeros((rows + 2 * HALO, 128 - 2 * HALO, layers), jnp.float32)
    side = jnp.transpose(jnp.concatenate([right, gap, left], 1), (0, 2, 1))
    diff = jnp.broadcast_to(
        jnp.pad(spreading_coefficient, (0, layers - fields))[:, None], (layers, 128))
    clipped = transport(main, top, bottom, side, diff, fields)
    tables = build_tables(colliding_pair, natural_exponent_scaler, arrhenius_energy,
                          stoichiometric_output, formation_warming, layers)
    reacted, warm = chemistry(clipped, by_count(explicit_increments), explicit_increments, tables)
    return reacted.reshape(species, rows, cols), warm


def solution(mesh):
    return jax.shard_map(
        body,
        mesh=mesh,
        in_specs=(
            P(None, "gx", "grp"),
            P("gx", "grp"),
            P("gx", "grp"),
            P("gx", "grp"),
            P(),
            P(),
            P(),
            P(),
            P(),
            P(),
            P(("grp", "gx")),
        ),
        out_specs=(P(None, "gx", "grp"), P("gx", "grp")),
        check_vma=False,
    )
```

```python
import functools
import math

import jax
import jax.numpy as jnp
import numpy as np
from jax import lax
from jax.experimental import pallas as pl
from jax.experimental.pallas import tpu as pltpu
from jax.sharding import PartitionSpec as P

TILE = 128
HALO = 9
FIRST_SCALE = 60.0
SECOND_SCALE = 180.0
transport_step = 0.4
chemistry_span = 0.5
sixth_first = (0.75, -0.15, 1.0 / 60.0)
sixth_second = (1.5, -0.15, 1.0 / 90.0)
sixth_center = -49.0 / 18.0


def up8(n):
    return -(-n // 8) * 8


def halo_kernel(sizes, main, first_cols, last_cols, top, bottom, left, right, send, recv):
    n_grp, n_gx = sizes
    g, x = lax.axis_index("grp"), lax.axis_index("gx")
    rows = main.shape[0]
    place = lambda dg, dx: (lax.rem(g + dg + n_grp, n_grp), lax.rem(x + dx + n_gx, n_gx))
    barrier = pltpu.get_barrier_semaphore()
    around = [(dg, dx) for dg in (-1, 0, 1) for dx in (-1, 0, 1) if (dg, dx) != (0, 0)]
    for dg, dx in around:
        pl.semaphore_signal(barrier, inc=1, device_id=place(dg, dx),
                            device_id_type=pl.DeviceIdType.MESH)
    pl.semaphore_wait(barrier, len(around))
    early, late = pl.ds(0, HALO), pl.ds(rows - HALO, HALO)
    above, beside, below = pl.ds(0, HALO), pl.ds(HALO, rows), pl.ds(HALO + rows, HALO)
    plan = [
        (main.at[late], top, 0, 1),
        (main.at[early], bottom, 0, -1),
        (last_cols, left.at[beside], 1, 0),
        (first_cols, right.at[beside], -1, 0),
        (last_cols.at[late], left.at[above], 1, 1),
        (last_cols.at[early], left.at[below], 1, -1),
        (first_cols.at[late], right.at[above], -1, 1),
        (first_cols.at[early], right.at[below], -1, -1),
    ]
    copies = []
    for n, (src, dst, dg, dx) in enumerate(plan):
        copy = pltpu.make_async_remote_copy(
            src_ref=src, dst_ref=dst, send_sem=send.at[n], recv_sem=recv.at[n],
            device_id=place(dg, dx), device_id_type=pl.DeviceIdType.MESH)
        copy.start()
        copies.append(copy)
    for copy in copies:
        copy.wait()


def exchange(main, first_cols, last_cols):
    rows, layers, cols = main.shape
    sizes = (lax.axis_size("grp"), lax.axis_size("gx"))
    anywhere = pl.BlockSpec(memory_space=pltpu.VMEM)
    strip = jax.ShapeDtypeStruct((HALO, layers, cols), jnp.float32)
    edge = jax.ShapeDtypeStruct((rows + 2 * HALO,) + first_cols.shape[1:], jnp.float32)
    return pl.pallas_call(
        functools.partial(halo_kernel, sizes),
        in_specs=[anywhere] * 3,
        out_specs=[anywhere] * 4,
        out_shape=[strip, strip, edge, edge],
        scratch_shapes=[pltpu.SemaphoreType.DMA((8,)), pltpu.SemaphoreType.DMA((8,))],
        compiler_params=pltpu.CompilerParams(collective_id=0, has_side_effects=True),
        name="halo",
    )(main, first_cols, last_cols)


def halves(value):
    high = value.astype(jnp.bfloat16)
    return high, (value - high.astype(jnp.float32)).astype(jnp.bfloat16)


def transport_kernel(fields, main, top, bottom, side, diff, band, uv_main, uv_top, uv_bottom, uv_side,
                     out, start, one, two, east, north, pieces, across):
    rows, _, cols = main.shape
    wide = rows + 2 * HALO
    gap = side.shape[2]
    width = cols + gap
    tile = pl.program_id(0)
    u_at, v_at = fields % 8, (fields + 1) % 8

    def fill(dst, m, t, b, s, sub):
        def put(r, ref, at):
            if sub is None:
                dst[r, :, :cols] = ref[at]
            else:
                dst[r, :, :cols] = jnp.broadcast_to(ref[at, sub:sub + 1, :], (8, cols))

        def mid(r, c):
            put(HALO + r, m, r)
            return c

        lax.fori_loop(0, rows, mid, 0, unroll=4)
        for r in range(HALO):
            put(r, t, r)
            put(HALO + rows + r, b, r)

        def edge(r, c):
            if sub is None:
                dst[r, :, cols:] = s[r]
            else:
                dst[r, :, cols:] = jnp.broadcast_to(s[r, sub:sub + 1, :], (8, gap))
            return c

        lax.fori_loop(0, wide, edge, 0, unroll=5)

    @pl.when(tile == 0)
    def _():
        fill(east, uv_main, uv_top, uv_bottom, uv_side, u_at)
        fill(north, uv_main, uv_top, uv_bottom, uv_side, v_at)

    fill(start, main, top, bottom, side, None)
    d = diff[...] * transport_step
    d_wide = jnp.concatenate([d] * (width // 128), axis=1)

    def columns(src, low, high):
        scale = d_wide * (1.0 / SECOND_SCALE)

        def split(j, c):
            fs, gs = [], []
            for q in range(2):
                i = low + 2 * j + q
                f = src[i]
                fs.append(scale * f)
                gs.append((-transport_step / FIRST_SCALE) * (north[i] * f))
            f_high, f_low = halves(jnp.concatenate(fs, 0))
            g_high, g_low = halves(jnp.concatenate(gs, 0))
            at = pl.ds(pl.multiple_of(j * 16, 16), 16)
            pieces[at, 0:width] = f_high
            pieces[at, width:2 * width] = f_low
            pieces[at, 2 * width:3 * width] = g_high
            pieces[at, 3 * width:4 * width] = g_low
            return c

        lax.fori_loop(0, (high - low) // 2, split, 0, unroll=2 if (high - low) % 4 == 0 else 1)
        count = (high - low) * 8
        across[0:count] = jnp.dot(pieces[0:count], band[...], preferred_element_type=jnp.float32)

    def change(src, i, low, n):
        lap = sixth_center * src[i, :, :n]
        grad = None
        for k in range(1, 4):
            ahead, behind = src[i + k, :, :n], src[i - k, :, :n]
            lap = lap + sixth_second[k - 1] * (ahead + behind)
            slope = (sixth_first[k - 1] * transport_step) * (
                east[i + k, :, :n] * ahead - east[i - k, :, :n] * behind)
            grad = slope if grad is None else grad + slope
        col = across[pl.ds(pl.multiple_of((i - low) * 8, 8), 8), :n]
        return col + (d_wide[:, :n] * lap - grad)

    columns(start, 3, wide - 3)

    def first(i, c):
        one[i] = start[i] + change(start, i, 3, width)
        return c

    lax.fori_loop(3, wide - 3, first, 0, unroll=2)
    columns(one, 6, wide - 6)

    def second(i, c):
        two[i] = 0.75 * start[i] + 0.25 * (one[i] + change(one, i, 6, width))
        return c

    lax.fori_loop(6, wide - 6, second, 0, unroll=2)
    columns(two, 9, wide - 9)
    ids = tile * 8 + lax.broadcasted_iota(jnp.int32, (8, cols), 0)
    is_species = ids < fields - 1

    def third(i, c):
        value = start[i, :, :cols] * (1.0 / 3.0) + (2.0 / 3.0) * (
            two[i, :, :cols] + change(two, i, 9, cols))
        out[i - HALO] = jnp.where(is_species, jnp.maximum(value, 0.0), value)
        return c

    lax.fori_loop(9, wide - 9, third, 0, unroll=2)


def band_matrix(width):
    here = np.arange(width)
    lag = (here[:, None] - here[None, :]) % width
    second = np.where(lag == 0, round(sixth_center * SECOND_SCALE), 0)
    first = np.zeros((width, width))
    for k in range(1, 4):
        ahead, behind = lag == k, lag == width - k
        second = np.where(ahead | behind, round(sixth_second[k - 1] * SECOND_SCALE), second)
        weight = round(sixth_first[k - 1] * FIRST_SCALE)
        first = np.where(ahead, weight, np.where(behind, -weight, first))
    return jnp.asarray(np.concatenate([second, second, first, first], 0), jnp.bfloat16)


def transport(main, top, bottom, side, vectors, diff_at, fields):
    rows, layers, cols = main.shape
    wide = rows + 2 * HALO
    gap = side.shape[2]
    width = cols + gap
    uv_tile = fields // 8
    band = band_matrix(width)
    by = lambda r, n: pl.BlockSpec((r, 8, n), lambda t: (0, t, 0))
    uv = lambda r, n: pl.BlockSpec((r, 8, n), lambda t: (0, uv_tile, 0))
    return pl.pallas_call(
        functools.partial(transport_kernel, fields),
        grid=(layers // 8,),
        in_specs=[by(rows, cols), by(HALO, cols), by(HALO, cols), by(wide, gap),
                  pl.BlockSpec((8, 128), lambda t: (diff_at + t, 0)),
                  pl.BlockSpec(band.shape, lambda t: (0, 0)),
                  uv(rows, cols), uv(HALO, cols), uv(HALO, cols), uv(wide, gap)],
        out_specs=by(rows, cols),
        out_shape=jax.ShapeDtypeStruct(main.shape, jnp.float32),
        scratch_shapes=[pltpu.VMEM((wide, 8, width), jnp.float32) for _ in range(5)]
        + [pltpu.VMEM(((wide - 6) * 8, 4 * width), jnp.bfloat16),
           pltpu.VMEM(((wide - 6) * 8, width), jnp.float32)],
        name="transport",
    )(main, top, bottom, side, vectors, band, main, top, bottom, side)


CHAINS = 2


def chemistry_kernel(reactions, warm_row, order, counts, state, gather, sums, vectors, out,
                     warm_out, staged, sems, *scratch):
    R = reactions
    rows, layers, cols = state.shape
    per_row = cols // TILE
    tiles = rows * per_row
    cells = 2 * TILE
    group = 2 * CHAINS
    is_warm = lax.broadcasted_iota(jnp.int32, (layers, 1), 0) == warm_row
    second_half = lax.broadcasted_iota(jnp.int32, (1, cells), 1) >= TILE
    values, partners, parts = scratch[:CHAINS], scratch[CHAINS:2 * CHAINS], scratch[2 * CHAINS:]

    def handle(g, c):
        ids = [order[g * group + t] for t in range(group)]
        places = [(t // per_row, pl.ds(pl.multiple_of((t % per_row) * TILE, TILE), TILE)) for t in ids]
        numbers = [counts[t] for t in ids]
        turn_count = functools.reduce(jnp.maximum, numbers)
        steps, cell_counts = [], []
        for q in range(CHAINS):
            n = jnp.where(second_half, numbers[2 * q + 1], numbers[2 * q])
            cell_counts.append(n)
            steps.append(chemistry_span / n.astype(jnp.float32))
            for t in range(2):
                r, at = places[2 * q + t]
                values[q][:, t * TILE:(t + 1) * TILE] = state[r, :, at]

        def advance(s, c):
            for q in range(CHAINS):
                high, low = halves(values[q][...])
                pieces = jnp.concatenate(
                    [high.astype(jnp.float32), low.astype(jnp.float32)], 0).astype(jnp.bfloat16)
                partners[q][...] = jnp.dot(gather[...], pieces, preferred_element_type=jnp.float32)
            for q in range(CHAINS):
                heat = jnp.tanh(values[q][warm_row:warm_row + 1, :])
                for r in range(0, R, 16):
                    block = pl.ds(r, 16)
                    a = jnp.concatenate([vectors[block]] * 2, 1)
                    e = jnp.concatenate([vectors[pl.ds(R + r, 16)]] * 2, 1)
                    rate = jnp.exp2(a + e * heat)
                    ca = partners[q][block]
                    cb = partners[q][pl.ds(R + r, 16)]
                    qa = rate * ca
                    qb = rate * cb
                    p = qa * cb
                    for n, value in enumerate((p, qb, qa)):
                        hi, lo = halves(value)
                        parts[q][pl.ds(2 * n * R + r, 16)] = hi
                        parts[q][pl.ds((2 * n + 1) * R + r, 16)] = lo
            for q in range(CHAINS):
                x = values[q][...]
                h = steps[q]
                both = jnp.dot(sums[0:2 * layers, 0:2 * R], parts[q][0:2 * R],
                               preferred_element_type=jnp.float32)
                destroyed = jnp.dot(sums[0:layers, 2 * R:], parts[q][2 * R:],
                                    preferred_element_type=jnp.float32)
                gained = both[:layers] + both[layers:]
                updated = (x + h * gained) / (1.0 + h * destroyed)
                change = jnp.sum(vectors[2 * R:2 * R + layers, 0:1] * (updated - x), axis=0, keepdims=True)
                updated = jnp.where(is_warm, x + change, updated)
                values[q][...] = jnp.where(s < cell_counts[q], updated, x)
            return c

        lax.fori_loop(0, turn_count, advance, 0)
        for q in range(CHAINS):
            for t in range(2):
                r, at = places[2 * q + t]
                done = values[q][:, t * TILE:(t + 1) * TILE]
                for f in range(0, layers, 8):
                    n = min(8, warm_row + 1 - f)
                    if n > 0:
                        staged[pl.ds(((ids[2 * q + t] % per_row) * (warm_row + 1) + f) * rows + r, n, stride=rows)] = done[f:f + n]
        return c

    lax.fori_loop(0, tiles // group, handle, 0)
    height = (warm_row + 1) * rows
    copies = []
    for n in range(per_row):
        at = pl.ds(n * TILE, TILE)
        copies.append(pltpu.make_async_copy(
            staged.at[pl.ds(n * height, warm_row * rows)], out.at[:, at], sems.at[0, n]))
        copies.append(pltpu.make_async_copy(
            staged.at[pl.ds(n * height + warm_row * rows, rows)], warm_out.at[:, at], sems.at[1, n]))
    for copy in copies:
        copy.start()
    for copy in copies:
        copy.wait()


def chemistry(state, order, counts, tables):
    rows, layers, cols = state.shape
    gather, sums, vectors, R, warm_row = tables
    smem = pl.BlockSpec(memory_space=pltpu.SMEM)
    vmem = pl.BlockSpec(memory_space=pltpu.VMEM)
    return pl.pallas_call(
        functools.partial(chemistry_kernel, R, warm_row),
        in_specs=[smem, smem] + [vmem] * 4,
        out_specs=[pl.BlockSpec(memory_space=pl.ANY)] * 2,
        out_shape=[jax.ShapeDtypeStruct((warm_row * rows, cols), jnp.float32),
                   jax.ShapeDtypeStruct((rows, cols), jnp.float32)],
        scratch_shapes=[pltpu.VMEM((cols // TILE * (warm_row + 1) * rows, TILE), jnp.float32),
                        pltpu.SemaphoreType.DMA((2, cols // TILE))]
        + [pltpu.VMEM((layers, 2 * TILE), jnp.float32)] * CHAINS
        + [pltpu.VMEM((2 * R, 2 * TILE), jnp.float32)] * CHAINS
        + [pltpu.VMEM((6 * R, 2 * TILE), jnp.bfloat16)] * CHAINS,
        name="chemistry",
    )(order, counts, state, gather, sums, vectors)


def by_count(counts):
    tiles = counts.shape[0]
    ids = jnp.arange(tiles, dtype=jnp.int32)
    key = counts * tiles + ids
    rank = jnp.sum((key[None, :] < key[:, None]).astype(jnp.int32), 1)
    return jnp.sum(jnp.where(rank[:, None] == ids[None, :], ids[:, None], 0), 0)


def build_tables(colliding_pair, produced, layers):
    reactions, species = produced.shape
    R = -(-reactions // 16) * 16
    pad = R - reactions
    ids = jnp.arange(layers, dtype=jnp.int32)
    pair = jnp.pad(colliding_pair, ((0, pad), (0, 0)), constant_values=-1)
    first = (pair[:, 0:1] == ids[None]).astype(jnp.bfloat16)
    second = (pair[:, 1:2] == ids[None]).astype(jnp.bfloat16)
    both = jnp.concatenate([first, second], 0)
    gather = jnp.concatenate([both, both], 1)
    gain = jnp.pad(produced.T, ((0, layers - species), (0, pad)))
    gain_high = lax.reduce_precision(gain, 8, 7)
    gain_low = (gain - gain_high).astype(jnp.bfloat16)
    gain_high = gain_high.astype(jnp.bfloat16)
    zero = jnp.zeros_like(gain_high)
    one = jnp.concatenate([gain_high, gain_high, first.T, first.T, second.T, second.T], 1)
    low = jnp.concatenate([gain_low, zero, zero, zero, zero, zero], 1)
    sums = jnp.concatenate([one, low], 0)
    return gather, sums, R


def body(component_density, scaled_thermal_state, leading_direction_flow, trailing_direction_flow,
         spreading_coefficient, colliding_pair, natural_exponent_scaler, arrhenius_energy,
         stoichiometric_output, formation_warming, explicit_increments):
    species, rows, cols = component_density.shape
    fields = species + 1
    layers = up8(fields + 2)
    bundle = jnp.concatenate(
        [component_density, scaled_thermal_state[None], leading_direction_flow[None],
         trailing_direction_flow[None]], 0)
    bundle = jnp.pad(bundle, ((0, layers - fields - 2), (0, 0), (0, 0)))
    main = jnp.transpose(bundle, (1, 0, 2))

    whole = lambda v: jnp.pad(
        jnp.transpose(v, (0, 2, 1)), ((0, 0), (0, up8(HALO) - HALO), (0, -layers % 128)))
    top, bottom, left, right = exchange(
        main, whole(main[:, :, :HALO]), whole(main[:, :, cols - HALO:]))
    gap = jnp.zeros((rows + 2 * HALO, 128 - 2 * HALO, layers), jnp.float32)
    side = jnp.transpose(
        jnp.concatenate([right[:, :HALO, :layers], gap, left[:, :HALO, :layers]], 1), (0, 2, 1))
    gather, sums, reactions = build_tables(colliding_pair, stoichiometric_output, layers)
    scale = 1.0 / math.log(2.0)
    fit = lambda v, n: jnp.pad(v, (0, n - v.shape[0]))
    vectors = jnp.concatenate(
        [fit(natural_exponent_scaler * scale, reactions), fit(arrhenius_energy * scale, reactions),
         fit(formation_warming, layers), fit(spreading_coefficient, layers)])
    vectors = jnp.broadcast_to(vectors[:, None], (vectors.shape[0], 128))
    clipped = transport(main, top, bottom, side, vectors, (2 * reactions + layers) // 8, fields)
    tables = (gather, sums, vectors, reactions, species)
    reacted, warm = chemistry(clipped, by_count(explicit_increments), explicit_increments, tables)
    return reacted.reshape(species, rows, cols), warm


def solution(mesh):
    return jax.shard_map(
        body,
        mesh=mesh,
        in_specs=(
            P(None, "gx", "grp"),
            P("gx", "grp"),
            P("gx", "grp"),
            P("gx", "grp"),
            P(),
            P(),
            P(),
            P(),
            P(),
            P(),
            P(("grp", "gx")),
        ),
        out_specs=(P(None, "gx", "grp"), P("gx", "grp")),
        check_vma=False,
    )
```
